32 devices in a mesh: rep: 4 (over x, y), dp: 8 (over z, core).
Axes of the slice: x: 2, y: 2, z: 4, core: 2. Of those that a mesh axis runs over, the one named last changes fastest.
Arguments:
- x: bfloat16 [32, 2048, 1024], P(('rep', 'dp')), parts along dimension 0
- dy: bfloat16 [32, 2048, 1024], P(('rep', 'dp')), parts along dimension 0
- w_gate: bfloat16 [2, 1024, 4096], replicated
- w_up: bfloat16 [2, 1024, 4096], replicated
- w_down: bfloat16 [2, 4096, 1024], replicated
- m_w_gate: float32 [2, 1024, 4096], replicated
- m_w_up: float32 [2, 1024, 4096], replicated
- m_w_down: float32 [2, 4096, 1024], replicated
- v_w_gate: float32 [2, 1024, 4096], replicated
- v_w_up: float32 [2, 1024, 4096], replicated
- v_w_down: float32 [2, 4096, 1024], replicated
Outputs:
- output 1: bfloat16 [8, 1024, 4096], P('rep'), parts along dimension 0
- output 2: bfloat16 [8, 1024, 4096], P('rep'), parts along dimension 0
- output 3: bfloat16 [8, 4096, 1024], P('rep'), parts along dimension 0
- output 4: float32 [8, 1024, 4096], P('rep'), parts along dimension 0
- output 5: float32 [8, 1024, 4096], P('rep'), parts along dimension 0
- output 6: float32 [8, 4096, 1024], P('rep'), parts along dimension 0
- output 7: float32 [8, 1024, 4096], P('rep'), parts along dimension 0
- output 8: float32 [8, 1024, 4096], P('rep'), parts along dimension 0
- output 9: float32 [8, 4096, 1024], P('rep'), parts along dimension 0
There are 4 independent parts. The reference program is written for one: setup_inputs(seed, part) draws one part's arguments, and reference() takes and returns one part's arrays. A program takes and returns all parts, laid end to end along the dimension named above; an argument that names none is the same for every part.
All inputs are finite; a program needn't handle non-finite values.
Results may differ from the reference program's by a relative error of at most 0.0237.
Values are sent between devices in bfloat16 or wider.
A program may use at most 2.75 GiB of HBM per device.

```python
import jax
import jax.numpy as jnp
from jax import lax

SEQUENCES = 8
TOKENS = 2048
D = 1024
FF = 4096
LAYERS = 2
NAMES = ("w_gate", "w_up", "w_down")
SHAPES = {"w_gate": (LAYERS, D, FF), "w_up": (LAYERS, D, FF), "w_down": (LAYERS, FF, D)}


def bump(key, n, height):
    away = (jnp.arange(n, dtype=jnp.int32) - jax.random.randint(key, (), 0, n, jnp.int32)) % n
    return jnp.where(away < n // 8, height, 1.0)


def together(key, own, strength):
    shared = jax.random.normal(key, own.shape[1:], jnp.float32)
    return (own + strength * shared) * lax.rsqrt(1 + strength * strength)


def setup_inputs(seed: int = 0, part: int = 0) -> dict:
    kx, kdy, ka, kb, kz, kf, kh, kl, *keys = jax.random.split(jax.random.key(seed), 8 + 3 * len(NAMES))
    kx, kdy, ka, kb = (jax.random.fold_in(k, part) for k in (kx, kdy, ka, kb))
    kw, km, kv = (keys[i::3] for i in range(3))
    shape = (SEQUENCES, TOKENS, D)
    much_x, much_dy = jax.random.uniform(kz, (2,), jnp.float32, 0.0, 1.0)
    loud = 2.0 ** jax.random.uniform(jax.random.fold_in(kz, 1), (), jnp.float32, -1.0, 2.0)
    layers = 2.0 ** jax.random.uniform(kl, (LAYERS, 1, 1), jnp.float32, -1.0, 1.0)
    x = together(ka, jax.random.normal(kx, shape, jnp.float32), much_x) * bump(kf, D, 4.0)
    dy = together(kb, jax.random.normal(kdy, shape, jnp.float32), much_dy)
    drawn = {"x": x.astype(jnp.bfloat16), "dy": (loud * dy * (SEQUENCES * TOKENS) ** -0.5).astype(jnp.bfloat16)}
    for key, name in zip(kw, NAMES, strict=True):
        w = jax.random.normal(key, SHAPES[name], jnp.float32) * SHAPES[name][1] ** -0.5
        drawn[name] = (w * {"w_gate": 1.0, "w_up": bump(kh, FF, 4.0), "w_down": layers}[name]).astype(jnp.bfloat16)
    for key, name in zip(km, NAMES, strict=True):
        drawn[f"m_{name}"] = 0.1 * jax.random.normal(key, SHAPES[name], jnp.float32)
    for key, name in zip(kv, NAMES, strict=True):
        drawn[f"v_{name}"] = jax.random.uniform(key, SHAPES[name], jnp.float32, 0.005, 0.015)
    return drawn


def matmul(a, w):
    return jnp.dot(a, w, preferred_element_type=jnp.float32).astype(jnp.bfloat16)


def normed(h):
    wide = h.astype(jnp.float32)
    scale = lax.rsqrt(jnp.mean(wide**2, -1, keepdims=True) + 1e-6)
    return (wide * scale).astype(jnp.bfloat16)


def layer(h, w):
    a = normed(h)
    gate = jnp.dot(a, w["w_gate"], preferred_element_type=jnp.float32)
    up = jnp.dot(a, w["w_up"], preferred_element_type=jnp.float32)
    return h + matmul((jax.nn.silu(gate) * up).astype(jnp.bfloat16), w["w_down"])


def adamw(w, m, v, g):
    m = 0.9 * m + 0.1 * g
    v = 0.95 * v + 0.05 * g * g
    step = m * lax.rsqrt(v + 1e-8) + 0.1 * w
    return (w - 0.02 * step).astype(jnp.bfloat16), m, v


def stack(weights, h):
    return lax.scan(lambda h, w: (layer(h, w), None), h, weights)[0]


def reference(x, dy, w_gate, w_up, w_down, m_w_gate, m_w_up, m_w_down, v_w_gate, v_w_up, v_w_down):
    weights = dict(zip(NAMES, (w_gate, w_up, w_down), strict=True))

    def take(so_far, sequence):
        h, by_y = sequence
        _, back = jax.vjp(lambda w: stack(w, h), weights)
        return jax.tree.map(lambda total, term: total + term.astype(jnp.float32), so_far, back(by_y)[0]), None

    none_yet = {name: jnp.zeros(w.shape, jnp.float32) for name, w in weights.items()}
    by_weights, _ = lax.scan(take, none_yet, (x, dy))
    gradients = [by_weights[name].astype(jnp.bfloat16).astype(jnp.float32) for name in NAMES]
    new = [
        adamw(w.astype(jnp.float32), m, v, g)
        for w, m, v, g in zip((w_gate, w_up, w_down), (m_w_gate, m_w_up, m_w_down), (v_w_gate, v_w_up, v_w_down), gradients, strict=True)
    ]
    return tuple(one[which] for which in range(3) for one in new)
```

```python
import jax
import jax.numpy as jnp
from jax import lax
from jax.experimental import pallas as pl
from jax.experimental.pallas import tpu as pltpu
from jax.sharding import PartitionSpec as P

F32 = jnp.float32
BF16 = jnp.bfloat16
T, D, FF = 2048, 1024, 4096
C = 256
J = FF // C
N = 6 * J
K = 12
HALF, QUARTER = D // 2, D // 4
ROWS = 1024
S1, S2, S3, S4, S5, S6, S7 = 1, 3, 5, 7, 9, 10, 11
NN = (((1,), (0,)), ((), ()))
NT = (((1,), (1,)), ((), ()))


def dot(a, b, dims=NN):
    return lax.dot_general(a, b, dims, preferred_element_type=F32)


def normalised(h):
    wide = h.astype(F32)
    return (wide * lax.rsqrt(jnp.mean(wide * wide, -1, keepdims=True) + 1e-6)).astype(BF16)


def tiles(total, size, body):
    @pl.loop(0, total // size)
    def _(i):
        body(pl.ds(pl.multiple_of(i * size, size), size))


def mega(x, dy, wg, wu, wd, h1, gs, a, at, dh, dht, acc, wgb, wub, wdb, act, dg, du, g, r0, r1, r2, full, wsem, csem, osem, *sems):
    s0s, s0r, s1s, s1r, s2s, s2r, s3s, s3r, s4s, s4r, s5s, s5r, s6s, s6r = sems
    me = lax.axis_index("dp")
    z, c = me // 2, me % 2
    end = (z == 0) | (z == 3)
    mid = (z == 1) | (z == 2)
    partner = 2 * z + (1 - c)
    inward = jnp.where(z == 0, 1, jnp.where(z == 1, 2, jnp.where(z == 2, 1, 2))) * 2 + c
    outward = jnp.where(z == 1, 0, 3) * 2 + c
    barrier = pltpu.get_barrier_semaphore()

    def hello(device):
        pl.semaphore_signal(barrier, inc=1, device_id={"dp": device}, device_id_type=pl.DeviceIdType.MESH)

    hello(partner)
    hello(inward)

    @pl.when(mid)
    def _():
        hello(outward)
        pl.semaphore_wait(barrier, 3)

    @pl.when(end)
    def _():
        pl.semaphore_wait(barrier, 2)

    def remote(src, dst, send, recv, device):
        return pltpu.make_async_remote_copy(
            src_ref=src, dst_ref=dst, send_sem=send, recv_sem=recv, device_id={"dp": device}, device_id_type=pl.DeviceIdType.MESH
        )

    def local(src, dst, sem):
        return pltpu.make_async_copy(src, dst, sem)

    def fetch(u):
        layer = jnp.where(u // J == 1, 1, 0)
        cols = pl.ds(pl.multiple_of(u % J * C, C), C)
        slot = u % 2
        return (
            local(wg.at[layer, :, cols], wgb.at[slot], wsem.at[0, slot]),
            local(wu.at[layer, :, cols], wub.at[slot], wsem.at[1, slot]),
            local(wd.at[layer, cols, :], wdb.at[slot], wsem.at[2, slot]),
        )

    def next_weights(u):
        @pl.when(u + 1 < 3 * J)
        def _():
            for copy in fetch(u + 1):
                copy.start()

        for copy in fetch(u):
            copy.wait()

    mine, other = c * HALF, (1 - c) * HALF
    own, away = (2 - z) * QUARTER, (z - 1) * QUARTER

    def at_row(row, size):
        return pl.ds(pl.multiple_of(row, QUARTER), size)

    def stage0(n):
        s = n % K
        return remote(g.at[s, at_row(other, HALF)], r0.at[s], s0s.at[s], s0r.at[s], partner)

    def stage1(n):
        s = n % K
        return remote(g.at[s, at_row(mine, HALF)], r1.at[s], s1s.at[s], s1r.at[s], inward)

    def stage2(n):
        s = n % K
        return remote(g.at[s, at_row(mine + away, QUARTER)], r2.at[s], s2s.at[s], s2r.at[s], inward)

    def stage3(n):
        s = n % K
        rows = full.at[s, at_row(mine + own, QUARTER)]
        return remote(rows, rows, s3s.at[s], s3r.at[s], inward)

    def stage4(n, row):
        s = n % K
        rows = full.at[s, at_row(row, QUARTER)]
        return remote(rows, rows, s4s.at[s], s4r.at[s], outward)

    def stage5(n, row):
        s = n % K
        rows = full.at[s, at_row(row, QUARTER)]
        return remote(rows, rows, s5s.at[s], s5r.at[s], outward)

    def stage6(n):
        s = n % K
        rows = full.at[s, at_row(mine, HALF)]
        return remote(rows, rows, s6s.at[s], s6r.at[s], partner)

    def result(n):
        s = n % K
        cols = pl.ds(pl.multiple_of(n // 3 % J * C, C), C)
        return local(full.at[s], gs.at[1 - n // (3 * J), n % 3, :, cols], osem.at[s])

    def live(n, also=None):
        ok = (n >= 0) & (n < N)
        return ok if also is None else ok & also

    def tick(t):
        @pl.when(live(t - S7))
        def _():
            result(t - S7).wait()

        @pl.when(live(t - S1))
        def _():
            n = t - S1
            s = n % K
            stage0(n).wait_recv()
            rows = at_row(mine, HALF)
            g[s, rows] = (g[s, rows].astype(F32) + r0[s].astype(F32)).astype(BF16)

            @pl.when(end)
            def _():
                stage1(n).start()

        @pl.when(live(t - S4, mid))
        def _():
            n = t - S4
            stage3(n).wait_recv()
            stage5(n, mine + away).start()

        @pl.when(live(t - S3, mid))
        def _():
            n = t - S3
            s = n % K
            stage2(n).wait()
            rows = at_row(mine + own, QUARTER)
            r = at_row(own, QUARTER)
            full[s, rows] = (g[s, rows].astype(F32) + r1[s, r].astype(F32) + r2[s].astype(F32)).astype(BF16)
            stage3(n).start()
            stage4(n, mine + own).start()

        @pl.when(live(t - S3, end))
        def _():
            stage1(t - S3).wait_send()

        @pl.when(live(t - S2, mid))
        def _():
            n = t - S2
            s = n % K
            stage1(n).wait_recv()
            rows = at_row(mine + away, QUARTER)
            g[s, rows] = (g[s, rows].astype(F32) + r1[s, at_row(away, QUARTER)].astype(F32)).astype(BF16)
            stage2(n).start()

        @pl.when(live(t - S2))
        def _():
            stage0(t - S2).wait_send()

        @pl.when(live(t - S5, end))
        def _():
            n = t - S5
            stage4(n, mine).wait_recv()
            stage5(n, mine).wait_recv()

        @pl.when(live(t - S5, mid))
        def _():
            n = t - S5
            stage3(n).wait_send()
            stage4(n, mine).wait_send()
            stage5(n, mine).wait_send()

        @pl.when(live(t - S5))
        def _():
            stage6(t - S5).start()

        @pl.when(live(t))
        def _():
            stage0(t).start()

        @pl.when(live(t - S6))
        def _():
            n = t - S6
            stage6(n).wait()
            result(n).start()

    for copy in fetch(0):
        copy.start()
    into_a = local(x.at[0], a, csem.at[0])
    into_dh = local(x.at[0], dh, csem.at[1])
    into_a.start()
    into_dh.start()
    into_a.wait()

    def norm_rows(s):
        a[s] = normalised(a[s])

    tiles(T, 256, norm_rows)
    acc[...] = jnp.zeros_like(acc)

    @pl.loop(0, J)
    def _(u):
        next_weights(u)
        slot = u % 2

        def rows(s):
            gate, up = dot(a[s], wgb[slot]), dot(a[s], wub[slot])
            act[s] = (gate * jax.nn.sigmoid(gate) * up).astype(BF16)
            acc[s] += dot(act[s], wdb[slot])

        tiles(T, ROWS, rows)

    into_dh.wait()

    def first_states(s):
        h = (dh[s].astype(F32) + acc[s].astype(BF16).astype(F32)).astype(BF16)
        dh[s] = h
        a[s] = normalised(h)
        acc[s] = jnp.zeros_like(acc[s])

    tiles(T, 256, first_states)
    keep = local(dh, h1, csem.at[0])
    keep.start()

    def turn(source, target):
        def cols(s):
            target[s] = source[:, s].T

        tiles(D, 256, cols)

    turn(a, at)
    keep.wait()
    into_dh = local(dy.at[0], dh, csem.at[1])
    into_dh.start()
    into_dh.wait()
    turn(dh, dht)

    @pl.loop(0, 2 * J)
    def _(it):
        next_weights(J + it)
        slot = it % 2

        @pl.when(it == J)
        def _():
            again = local(h1, a, csem.at[0])
            again.start()
            again.wait()

            def rows(s):
                wide = a[s].astype(F32)
                d = acc[s].astype(BF16).astype(F32)
                scale = lax.rsqrt(jnp.mean(wide * wide, -1, keepdims=True) + 1e-6)
                along = jnp.sum(d * wide, -1, keepdims=True)
                d = (scale * d - wide * (scale * scale * scale * (1.0 / D) * along)).astype(BF16)
                dh[s] = (dh[s].astype(F32) + d.astype(F32)).astype(BF16)

            tiles(T, 256, rows)
            again = local(x.at[0], a, csem.at[0])
            again.start()
            turn(dh, dht)
            again.wait()
            tiles(T, 256, norm_rows)
            turn(a, at)

        def rows(s):
            gate, up = dot(a[s], wgb[slot]), dot(a[s], wub[slot])
            d = dot(dh[s], wdb[slot], NT).astype(BF16).astype(F32)
            sig = jax.nn.sigmoid(gate)
            silu = gate * sig
            act[s] = (silu * up).astype(BF16)
            du[s] = (d * silu).astype(BF16)
            dg[s] = (d * up * (sig * (1.0 + gate * (1.0 - sig)))).astype(BF16)

        tiles(T, ROWS, rows)
        tick(3 * it - 1)
        base = it % 4 * 3
        g[base] = dot(dht[...], act[...]).astype(BF16)
        g[base + 1] = dot(at[...], dg[...]).astype(BF16)
        g[base + 2] = dot(at[...], du[...]).astype(BF16)
        tick(3 * it)

        @pl.when(it < J)
        def _():
            def rows(s):
                acc[s] += dot(dg[s], wgb[slot], NT) + dot(du[s], wub[slot], NT)

            tiles(T, ROWS, rows)

        tick(3 * it + 1)

    @pl.loop(N - 1, N + S7)
    def _(t):
        tick(t)


def gradients(x, dy, wg, wu, wd):
    anywhere = pl.BlockSpec(memory_space=pl.ANY)
    sem = pltpu.SemaphoreType.DMA
    vm = pltpu.VMEM
    return pl.pallas_call(
        mega,
        out_shape=(jax.ShapeDtypeStruct((T, D), BF16), jax.ShapeDtypeStruct((2, 3, D, FF), BF16)),
        in_specs=[anywhere] * 5,
        out_specs=(anywhere, anywhere),
        scratch_shapes=[
            vm((T, D), BF16), vm((D, T), BF16), vm((T, D), BF16), vm((D, T), BF16), vm((T, D), F32),
            vm((2, D, C), BF16), vm((2, D, C), BF16), vm((2, C, D), BF16),
            vm((T, C), BF16), vm((T, C), BF16), vm((T, C), BF16),
            vm((K, D, C), BF16), vm((K, HALF, C), BF16), vm((K, HALF, C), BF16), vm((K, QUARTER, C), BF16), vm((K, D, C), BF16),
            sem((3, 2)), sem((2,)), sem((K,)),
        ] + [sem((K,))] * 14,
        compiler_params=pltpu.CompilerParams(collective_id=0, has_side_effects=True, vmem_limit_bytes=67043328),
        name="gradients",
    )(x, dy, wg, wu, wd)


def adam_body(turned, g, w, m, v, ow, om, ov):
    gg = g[0, 0].T if turned else g[0, 0]
    gg = gg.astype(F32)
    mm = 0.9 * m[0] + 0.1 * gg
    vv = 0.95 * v[0] + 0.05 * gg * gg
    ww = w[0].astype(F32)
    ow[0] = (ww - 0.02 * (mm * lax.rsqrt(vv + 1e-8) + 0.1 * ww)).astype(BF16)
    om[0] = mm
    ov[0] = vv


def adam(which, gs, w, m, v):
    down = which == 0
    if down:
        rows, cols = 256, D
        gspec = pl.BlockSpec((1, 1, D, rows), lambda l, i: (l, which, 0, i))
    else:
        rows, cols = 64, FF
        gspec = pl.BlockSpec((1, 1, rows, FF), lambda l, i: (l, which, i, 0))
    spec = pl.BlockSpec((1, rows, cols), lambda l, i: (l, i, 0))
    return pl.pallas_call(
        lambda *refs: adam_body(down, *refs),
        grid=(2, w.shape[1] // rows),
        in_specs=[gspec, spec, spec, spec],
        out_specs=[spec] * 3,
        out_shape=[jax.ShapeDtypeStruct(w.shape, t) for t in (BF16, F32, F32)],
        name="adam",
    )(gs, w, m, v)


def solution(mesh):
    def step(x, dy, wg, wu, wd, mg, mu, md, vg, vu, vd):
        _, gs = gradients(x, dy, wg, wu, wd)
        new = [adam(1, gs, wg, mg, vg), adam(2, gs, wu, mu, vu), adam(0, gs, wd, md, vd)]
        return tuple(new[i][which] for which in range(3) for i in range(3))

    return jax.shard_map(
        step,
        mesh=mesh,
        in_specs=(P(("rep", "dp"), None, None),) * 2 + (P(None, None, None),) * 9,
        out_specs=(P("rep", None, None),) * 9,
        check_vma=False,
    )
```
